32 devices in a mesh: py: 4 (over y, x), pz: 8 (over z, core).
Axes of the slice: x: 2, y: 2, z: 4, core: 2. Of those that a mesh axis runs over, the one named last changes fastest.
Arguments:
- species: float32 [4, 512, 64, 64], P(None, None, 'py', 'pz'), may hold values from -6 to 6
- coupling: float32 [4, 4], replicated, may hold values from -4 to 4
- symbol_x: float32 [512], replicated, may hold values from 0.3 to 3
- symbol_y: float32 [64], replicated, may hold values from 0.3 to 3
- symbol_z: float32 [64], replicated, may hold values from 0.3 to 3
Outputs:
- modes: float32 [4, 512, 64, 64], P(None, 'py', 'pz')
The draws below stay inside these ranges and needn't reach their ends.
All inputs are finite; a program needn't handle non-finite values.
Results may differ from the reference program's by a relative error of at most 0.00007.
Values sent between devices are 32-bit elements; how exact they have to be, the bound alone decides.
No kernel may reach another device: no remote copies, remote signals or barrier semaphores. Data moves between devices by JAX's collectives and lax.ppermute only.
A program may use at most 64 MiB of HBM per device.

```python
import jax
import jax.numpy as jnp
from jax import lax

GRID_X = 512
GRID_Y = 64
GRID_Z = 64
FIELDS = 4


def block_levels(key, shape, pieces, low, largest):
    def one(dim, shards_of):
        draws = jax.random.uniform(jax.random.fold_in(jax.random.fold_in(key, 6), dim), (shards_of,), jnp.float32, low / len(pieces), largest / len(pieces))
        return jnp.repeat(jnp.exp(draws), shape[dim] // shards_of).reshape((-1,) + (1,) * (len(shape) - dim - 1))

    gain = one(*pieces[0])
    for cut in pieces[1:]:
        gain = gain * one(*cut)
    return gain


def bell_draw(rng, shape, spread, most, shards=(), dtype=jnp.bfloat16):
    result = spread * jax.random.normal(rng, shape, jnp.float32)
    if shards:
        result = result * block_levels(rng, shape, shards, -0.22, 0.18)
    return jnp.clip(result, -most, most).astype(dtype)


def setup_inputs(seed: int = 0) -> dict:
    key_list = jax.random.split(jax.random.key(seed), 6)
    return {
        "species": bell_draw(key_list[0], (FIELDS, GRID_X, GRID_Y, GRID_Z), 1.0, 6.0, ((2, 4), (3, 8)), jnp.float32),
        "coupling": bell_draw(key_list[1], (FIELDS, FIELDS), 0.7, 4.0, (), jnp.float32),
        "symbol_x": jnp.clip(jax.random.uniform(key_list[2], (GRID_X,), jnp.float32, 0.3, 3.0), 0.3, 3.0),
        "symbol_y": jnp.clip(jax.random.uniform(key_list[3], (GRID_Y,), jnp.float32, 0.3, 3.0), 0.3, 3.0),
        "symbol_z": jnp.clip(jax.random.uniform(key_list[4], (GRID_Z,), jnp.float32, 0.3, 3.0), 0.3, 3.0),
    }


def mode_table(count):
    rank = jnp.arange(count)
    angle = (jnp.pi / (4 * count)) * (((2 * rank[:, None] + 1) * (2 * rank[None, :] + 1)) % (8 * count)).astype(jnp.float32)
    return jnp.cos(angle) * (2.0 / count) ** 0.5


def transform_dim(values, dim):
    moved = jnp.tensordot(values, mode_table(values.shape[dim]), axes=([dim], [0]), precision=lax.Precision.HIGHEST)
    return jnp.moveaxis(moved, -1, dim)


def reference(species, coupling, symbol_x, symbol_y, symbol_z):
    modes = species
    modes = transform_dim(modes, 1)
    modes = transform_dim(modes, 2)
    modes = transform_dim(modes, 3)
    symbol = symbol_x[:, None, None] + symbol_y[None, :, None] + symbol_z[None, None, :]
    weight_xyz = 1.0 / (1.0 + symbol)
    mixed_fields = jnp.einsum("ab,bxyz->axyz", coupling, modes, precision=lax.Precision.HIGHEST)
    modes = weight_xyz * modes + (1.0 - weight_xyz) * mixed_fields
    return modes
```

```python
import functools

import jax
import jax.numpy as jnp
import numpy as np
from jax import lax
from jax.experimental import pallas as pl
from jax.experimental.pallas import tpu as pltpu
from jax.sharding import PartitionSpec as P

CHUNKS = ((0, 2), (2, 2))
BF16, F32 = jnp.bfloat16, jnp.float32
VMEM = pl.BlockSpec(memory_space=pltpu.VMEM)


def mode_table(count):
    rank = np.arange(count)
    angle = np.pi / (4 * count) * ((2 * rank[:, None] + 1) * (2 * rank[None, :] + 1) % (8 * count))
    return np.cos(angle) * (2.0 / count) ** 0.5


def halves(table):
    high = table.astype(BF16)
    return np.stack([high, (table - high.astype(np.float64)).astype(BF16)])


def split(values):
    high = values.astype(BF16)
    return high, (values - high.astype(F32)).astype(BF16)


def dot(a, b):
    return jnp.dot(a, b, preferred_element_type=F32)


def dot3(a, b):
    return dot(a[0], b[0]) + (dot(a[0], b[1]) + dot(a[1], b[0]))


def call(body, outs, name, scratch=(), flops=0, **more):
    return pl.pallas_call(
        body,
        out_shape=outs,
        scratch_shapes=list(scratch),
        name=name,
        cost_estimate=pl.CostEstimate(flops=flops, bytes_accessed=1 << 20, transcendentals=0),
        compiler_params=pltpu.CompilerParams(vmem_limit_bytes=24 << 20),
        **more,
    )


def along_x(values, table, first, fields, parts):
    rows, width = values.shape[1:]
    part = width // parts

    def body(v_ref, h_ref, *refs):
        outs, r_ref = refs[:parts], refs[parts]
        modes = dot3(split(v_ref[0]), (h_ref[0], h_ref[1]))
        for j in range(parts):
            r_ref[j] = modes[:, j * part:(j + 1) * part]
        me = lax.axis_index("py")
        for k in range(parts):
            outs[k][0] = r_ref[me ^ k]

    spec = pl.BlockSpec((1, rows, part), lambda i: (i, 0, 0))
    return call(
        body,
        [jax.ShapeDtypeStruct((fields, rows, part), F32)] * parts,
        "along_x",
        [pltpu.VMEM((parts, rows, part), F32)],
        6 * fields * rows * width * width,
        grid=(fields,),
        in_specs=[pl.BlockSpec((1, rows, width), lambda i: (first + i, 0, 0)), pl.BlockSpec(table.shape, lambda i: (0, 0, 0))],
        out_specs=[spec] * parts,
    )(values, table)


def along_y(arrived, table, wanted, parts):
    sets, sources = len(arrived), len(arrived[0])
    fields, rows, lanes = arrived[0][0].shape
    total = sum(a[0].shape[0] for a in arrived)
    height = sources * rows // parts

    def body(*refs):
        ins = refs[:sets * sources]
        h_ref = refs[sets * sources]
        outs = refs[sets * sources + 1:-2]
        hi_ref, lo_ref = refs[-2:]
        me_y, me_z = lax.axis_index("py"), lax.axis_index("pz")
        at = 0
        for s in range(sets):
            for f in range(ins[s * sources].shape[0]):
                for k in range(sources):
                    hi, lo = split(ins[s * sources + k][f])
                    where = pl.ds(pl.multiple_of((me_y ^ k) * rows, rows), rows)
                    hi_ref[where, at * lanes:(at + 1) * lanes] = hi
                    lo_ref[where, at * lanes:(at + 1) * lanes] = lo
                at += 1
        values = hi_ref[...], lo_ref[...]
        for n, k in enumerate(wanted):
            modes = dot3((h_ref[0, me_z ^ k], h_ref[1, me_z ^ k]), values)
            for f in range(total):
                outs[n][f] = modes[:, f * lanes:(f + 1) * lanes]

    return call(
        body,
        [jax.ShapeDtypeStruct((total, height, lanes), F32)] * len(wanted),
        "along_y",
        [pltpu.VMEM((sources * rows, total * lanes), BF16)] * 2,
        6 * len(wanted) * height * sources * rows * total * lanes,
        in_specs=[VMEM] * (sets * sources + 1),
        out_specs=[VMEM] * len(wanted),
    )(*[a for s in arrived for a in s], table)


def along_z(near, far, table, weight, coupling, chunks, parts):
    half = parts // 2
    fields, rows, lanes = near[0].shape
    share_y = weight.shape[0]
    share_z = rows // share_y
    width = parts * share_z

    def body(*refs):
        near_refs = refs[:half]
        far_refs = refs[half:half + half * len(chunks)]
        h_ref, w_ref, c_ref, out_ref, s_ref = refs[half + half * len(chunks):]
        me = lax.axis_index("pz")
        for k in range(half):
            for f in range(fields):
                s_ref[f, :, me ^ k] = near_refs[k][f].reshape(share_y, share_z, lanes)
        for n, (first, count) in enumerate(chunks):
            for k in range(half):
                for f in range(count):
                    s_ref[first + f, :, me ^ (half + k)] = far_refs[n * half + k][f].reshape(share_y, share_z, lanes)
        h = h_ref[0], h_ref[1]
        for y in range(share_y):
            values = s_ref[:, y].reshape(fields * width, lanes)
            old = dot3(h, split(values)).reshape(fields, width, lanes)
            w = w_ref[y]
            for a in range(fields):
                mixed = c_ref[a, 0] * old[0]
                for b in range(1, fields):
                    mixed = mixed + c_ref[a, b] * old[b]
                out_ref[a, y] = mixed + w * (old[a] - mixed)

    return call(
        body,
        jax.ShapeDtypeStruct((fields, share_y, width, lanes), F32),
        "along_z",
        [pltpu.VMEM((fields, share_y, parts, share_z, lanes), F32)],
        6 * fields * share_y * width * width * lanes * fields,
        in_specs=[VMEM] * (half + half * len(chunks) + 2) + [pl.BlockSpec(memory_space=pltpu.SMEM)],
        out_specs=VMEM,
    )(*near, *[a for s in far for a in s], table, weight, coupling)


def transform_dim(values, dim):
    table = jnp.asarray(mode_table(values.shape[dim]), F32)
    moved = jnp.tensordot(values, table, axes=([dim], [0]), precision=lax.Precision.HIGHEST)
    return jnp.moveaxis(moved, -1, dim)


def own_weight(symbol_x, symbol_y, symbol_z, share_x, share_y):
    part_x = lax.dynamic_slice_in_dim(symbol_x, lax.axis_index("py") * share_x, share_x)
    part_y = lax.dynamic_slice_in_dim(symbol_y, lax.axis_index("pz") * share_y, share_y)
    symbol = part_x[None, None, :] + part_y[:, None, None] + symbol_z[None, :, None]
    return 1.0 / (1.0 + symbol)


def whole_shards(species, coupling, symbol_x, symbol_y, symbol_z):
    values = transform_dim(species, 1)
    values = lax.all_to_all(values, "py", split_axis=1, concat_axis=2, tiled=True)
    values = transform_dim(values, 2)
    values = lax.all_to_all(values, "pz", split_axis=2, concat_axis=3, tiled=True)
    values = transform_dim(values, 3)
    weight = own_weight(symbol_x, symbol_y, symbol_z, values.shape[1], values.shape[2])
    weight = weight.transpose(2, 0, 1)
    mixed = jnp.einsum("ab,bxyz->axyz", coupling, values, precision=lax.Precision.HIGHEST)
    return weight * values + (1.0 - weight) * mixed


def shards(species, coupling, symbol_x, symbol_y, symbol_z, py, pz):
    fields, size_x, share_y, share_z = species.shape
    size_y, size_z = share_y * py, share_z * pz
    if size_y * share_z > 512 or py != 4 or pz != 8 or share_z % 8 or size_x % (128 * py):
        return whole_shards(species, coupling, symbol_x, symbol_y, symbol_z)
    values = species.transpose(0, 2, 3, 1).reshape(fields, share_y * share_z, size_x)
    table_x = halves(mode_table(size_x))
    table_y = halves(np.kron(mode_table(size_y), np.eye(share_z))).reshape(2, pz, -1, size_y * share_z)
    table_z = halves(np.kron(np.eye(fields), mode_table(size_z)))

    def swap(value, axis, count, k):
        return lax.ppermute(value, axis, [(i, i ^ k) for i in range(count)])

    arrived = []
    for first, count in CHUNKS:
        parts = along_x(values, table_x, first, count, py)
        arrived.append([parts[0]] + [swap(parts[k], "py", py, k) for k in range(1, py)])
    half = pz // 2
    far = []
    for block in arrived:
        parts = along_y([block], table_y, range(half, pz), pz)
        far.append([swap(parts[k], "pz", pz, half + k) for k in range(half)])
    parts = along_y(arrived, table_y, range(half), pz)
    near = [parts[0]] + [swap(parts[k], "pz", pz, k) for k in range(1, half)]

    weight = own_weight(symbol_x, symbol_y, symbol_z, size_x // py, size_y // pz)
    out = along_z(near, far, table_z, weight, coupling, CHUNKS, pz)
    return out.transpose(0, 3, 1, 2)


def solution(mesh):
    py, pz = mesh.shape["py"], mesh.shape["pz"]
    return jax.shard_map(
        functools.partial(shards, py=py, pz=pz),
        mesh=mesh,
        in_specs=(P(None, None, "py", "pz"), P(), P(), P(), P()),
        out_specs=P(None, "py", "pz", None),
        check_vma=False,
    )
```

```python
import jax
import jax.numpy as jnp
import numpy as np
from jax import lax
from jax.experimental import pallas as pl
from jax.experimental.pallas import tpu as pltpu
from jax.sharding import PartitionSpec as P


CHUNKS = ((0, 2, 'relay'), (2, 2, 'gather'))
PIECES = 2
BF16, F32 = jnp.bfloat16, jnp.float32
VMEM = pl.BlockSpec(memory_space=pltpu.VMEM)


def mode_table(count):
    rank = np.arange(count)
    angle = np.pi / (4 * count) * ((2 * rank[:, None] + 1) * (2 * rank[None, :] + 1) % (8 * count))
    return np.cos(angle) * (2.0 / count) ** 0.5


def halves(table):
    high = table.astype(BF16)
    return np.stack([high, (table - high.astype(np.float64)).astype(BF16)])


def split(values):
    high = values.astype(BF16)
    return high, (values - high.astype(F32)).astype(BF16)


def dot(a, b):
    return jnp.dot(a, b, preferred_element_type=F32)


def stack_left(table):
    high, low = halves(table)
    return np.concatenate([high, high, low], axis=1)


def call(body, outs, scratch=(), flops=0, limit=24 << 20, **more):
    return pl.pallas_call(
        body,
        out_shape=outs,
        scratch_shapes=list(scratch),
        cost_estimate=pl.CostEstimate(flops=flops, bytes_accessed=1 << 20, transcendentals=0),
        compiler_params=pltpu.CompilerParams(vmem_limit_bytes=limit),
        **more,
    )


def along_x(values, table, first, fields, parts, load):
    rows, width = values.shape[1:]
    part = width // parts
    pieces = PIECES if load else 1
    depth = width // pieces

    def body(v_ref, h_ref, *refs):
        outs = refs[:parts]
        v_own, r_ref, sems = refs[-3:]
        copies = []
        for n in range(pieces):
            at = pl.ds(n * depth, depth)
            copies.append([pltpu.make_async_copy(
                v_ref.at[pl.ds(first, fields), :, at], v_own.at[:, :, at], sems.at[0, n])])
            if load:
                copies[n].append(pltpu.make_async_copy(
                    h_ref.at[:, at], refs[parts].at[:, at], sems.at[1, n]))
        for piece in copies:
            for copy in piece:
                copy.start()
        table_ref = refs[parts] if load else h_ref
        modes = 0.0
        for n in range(pieces):
            for copy in copies[n]:
                copy.wait()
            at = slice(n * depth, (n + 1) * depth)
            high, low = split(v_own[:, :, at].reshape(fields * rows, depth))
            modes += dot(high, table_ref[0, at]) + dot(low, table_ref[0, at]) + dot(high, table_ref[1, at])
        for j in range(parts):
            r_ref[j] = modes[:, j * part:(j + 1) * part].reshape(fields, rows, part)
        me = lax.axis_index("py")
        for k in range(parts):
            outs[k][...] = r_ref[me ^ k]

    outs = [jax.ShapeDtypeStruct((fields, rows, part), F32)] * parts
    scratch = [
        pltpu.VMEM((fields, rows, width), F32),
        pltpu.VMEM((parts, fields, rows, part), F32),
        pltpu.SemaphoreType.DMA((2, pieces) if load else (1, pieces)),
    ]
    space = VMEM
    values = pltpu.with_memory_space_constraint(values, pltpu.HBM)
    if load:
        outs.append(jax.ShapeDtypeStruct(table.shape, BF16))
        table = pltpu.with_memory_space_constraint(table, pltpu.HBM)
        space = pl.BlockSpec(memory_space=pltpu.HBM)
    return call(
        body,
        outs,
        scratch,
        6 * fields * rows * width * width,
        in_specs=[pl.BlockSpec(memory_space=pltpu.HBM), space],
        out_specs=[VMEM] * len(outs),
    )(values, table)


def along_y(arrived, table, share_z, parts, outs):
    sources = len(arrived)
    fields, rows, lanes = arrived[0].shape
    share_y = rows // share_z
    size_y = sources * share_y
    out_y = size_y // parts

    def body(*refs):
        ins, h_ref = refs[:sources], refs[sources]
        out_refs = refs[sources + 1:-2]
        b_ref, r_ref = refs[-2:]
        me_y, me_z = lax.axis_index("py"), lax.axis_index("pz")
        for k in range(sources):
            start = (me_y ^ k) * share_y
            where = [pl.ds(pl.multiple_of(n * size_y + start, 16), share_y) for n in range(3)]
            for f in range(fields):
                for z in range(share_z):
                    high, low = split(ins[k][f, pl.ds(z, share_y, stride=share_z), :])
                    at = slice((f * share_z + z) * lanes, (f * share_z + z + 1) * lanes)
                    b_ref[where[0], at] = high
                    b_ref[where[1], at] = low
                    b_ref[where[2], at] = high
        r_ref[...] = dot(h_ref[...], b_ref[...])
        for blocks, ref in zip(outs, out_refs):
            for n, k in enumerate(blocks):
                where = pl.ds(pl.multiple_of((me_z ^ k) * out_y, 8), out_y)
                for f in range(fields):
                    for z in range(share_z):
                        at = slice((f * share_z + z) * lanes, (f * share_z + z + 1) * lanes)
                        ref[n, f, pl.ds(z, out_y, stride=share_z), :] = r_ref[where, at]

    wide = fields * share_z * lanes
    return call(
        body,
        [jax.ShapeDtypeStruct((len(blocks), fields, out_y * share_z, lanes), F32) for blocks in outs],
        [pltpu.VMEM((3 * size_y, wide), BF16), pltpu.VMEM((size_y, wide), F32)],
        6 * size_y * size_y * wide,
        in_specs=[VMEM] * (sources + 1),
        out_specs=[VMEM] * len(outs),
    )(*arrived, table)


def pack(outs):
    arrays = []
    for parts in outs:
        arrays += [a for a, _ in parts if not any(a is b for b in arrays)]
    place = [[([a is b for b in arrays].index(True), i) for a, i in parts] for parts in outs]

    def body(*refs):
        for parts, ref in zip(place, refs[len(arrays):]):
            for n, (a, i) in enumerate(parts):
                ref[n] = refs[a][i]

    return call(
        body,
        [jax.ShapeDtypeStruct((len(parts), *parts[0][0].shape[1:]), F32) for parts in outs],
        in_specs=[VMEM] * len(arrays),
        out_specs=[VMEM] * len(outs),
    )(*arrays)


def distinct(blocks):
    arrays = []
    for array, *_ in blocks:
        if not any(array is b for b in arrays):
            arrays.append(array)
    return arrays, [([array is b for b in arrays].index(True), *rest) for array, *rest in blocks]


def gather_z(place, ins, s_ref, share_y, share_z):
    me = lax.axis_index("pz")
    lanes = ins[0].shape[-1]
    for a, index, k, first in place:
        where = pl.ds(pl.multiple_of((me ^ k) * share_z, 8), share_z)
        for f in range(ins[a].shape[1]):
            lane = slice((first + f) * lanes, (first + f + 1) * lanes)
            s_ref[:, where, lane] = ins[a][index, f].reshape(share_y, share_z, lanes)


def modes_z(h_ref, values):
    high, low = split(values)
    return dot(h_ref[...], jnp.concatenate([high, low, high], axis=0))


def along_z(blocks, table, weight, coupling, fields):
    arrays, place = distinct(blocks)
    rows, lanes = arrays[0].shape[2:]
    share_y, width = weight.shape[:2]
    count = max(first + array.shape[1] for array, _, _, first in blocks)

    def body(*refs):
        ins = refs[:len(arrays)]
        h_ref, w_ref, c_ref, out_ref, s_ref = refs[len(arrays):]
        gather_z(place, ins, s_ref, share_y, rows // share_y)
        for y in range(share_y):
            modes = modes_z(h_ref, s_ref[y])
            old = [modes[:, n * lanes:(n + 1) * lanes] for n in range(count)]
            w = w_ref[y]
            for a in range(fields):
                mixed = scaled(c_ref, a, 0, old[0])
                for b in range(1, count):
                    mixed = mixed + scaled(c_ref, a, b, old[b])
                mixed = mixed - w * mixed
                out_ref[a, y] = mixed + w * old[a] if a < count else mixed

    return call(
        body,
        jax.ShapeDtypeStruct((fields, share_y, width, lanes), F32),
        [pltpu.VMEM((share_y, width, count * lanes), F32)],
        6 * share_y * width * width * lanes * count,
        in_specs=[VMEM] * (len(arrays) + 3),
        out_specs=VMEM,
    )(*arrays, table, weight, coupling)


def scaled(c_ref, a, b, values):
    tile = c_ref[a, b]
    return (values.reshape(-1, *tile.shape) * tile[None]).reshape(values.shape)


def along_z_and_mix(blocks, table, early, weight, coupling):
    arrays, place = distinct(blocks)
    rows, lanes = arrays[0].shape[2:]
    fields, share_y, width = early.shape[:3]
    start = min(first for *_, first in blocks)
    place = [(a, index, k, first - start) for a, index, k, first in place]

    def body(*refs):
        ins = refs[:len(arrays)]
        h_ref, e_ref, w_ref, c_ref, out_ref, s_ref, o_ref, sems = refs[len(arrays):]
        gather_z(place, ins, s_ref, share_y, rows // share_y)
        copies = []
        for y in range(share_y):
            modes = modes_z(h_ref, s_ref[y])
            old = [modes[:, n * lanes:(n + 1) * lanes] for n in range(fields - start)]
            w = w_ref[y]
            for a in range(fields):
                mixed = scaled(c_ref, a, start, old[0])
                for b in range(start + 1, fields):
                    mixed = mixed + scaled(c_ref, a, b, old[b - start])
                mixed = mixed - w * mixed
                if a >= start:
                    mixed = mixed + w * old[a - start]
                o_ref[a, y] = e_ref[a, y] + mixed
            copies.append(pltpu.make_async_copy(o_ref.at[:, y], out_ref.at[:, y], sems.at[y]))
            copies[-1].start()
        for copy in copies:
            copy.wait()

    return call(
        body,
        jax.ShapeDtypeStruct((fields, share_y, width, lanes), F32),
        [
            pltpu.VMEM((share_y, width, (fields - start) * lanes), F32),
            pltpu.VMEM((fields, share_y, width, lanes), F32),
            pltpu.SemaphoreType.DMA((share_y,)),
        ],
        6 * share_y * width * width * lanes * (fields - start),
        in_specs=[VMEM] * (len(arrays) + 4),
        out_specs=pl.BlockSpec(memory_space=pltpu.HBM),
    )(*arrays, table, early, weight, coupling)


def transform_dim(values, dim):
    table = jnp.asarray(mode_table(values.shape[dim]), F32)
    moved = jnp.tensordot(values, table, axes=([dim], [0]), precision=lax.Precision.HIGHEST)
    return jnp.moveaxis(moved, -1, dim)


def own_weight(symbol_x, symbol_y, symbol_z, share_x, share_y):
    part_x = lax.dynamic_slice_in_dim(symbol_x, lax.axis_index("py") * share_x, share_x)
    part_y = lax.dynamic_slice_in_dim(symbol_y, lax.axis_index("pz") * share_y, share_y)
    symbol = part_x[None, None, :] + part_y[:, None, None] + symbol_z[None, :, None]
    return 1.0 / (1.0 + symbol)


def whole_shards(species, coupling, symbol_x, symbol_y, symbol_z):
    values = transform_dim(species, 1)
    values = lax.all_to_all(values, "py", split_axis=1, concat_axis=2, tiled=True)
    values = transform_dim(values, 2)
    values = lax.all_to_all(values, "pz", split_axis=2, concat_axis=3, tiled=True)
    values = transform_dim(values, 3)
    weight = own_weight(symbol_x, symbol_y, symbol_z, values.shape[1], values.shape[2])
    weight = weight.transpose(2, 0, 1)
    mixed = jnp.einsum("ab,bxyz->axyz", coupling, values, precision=lax.Precision.HIGHEST)
    return weight * values + (1.0 - weight) * mixed


def shards(species, coupling, symbol_x, symbol_y, symbol_z, py, pz):
    fields, size_x, share_y, share_z = species.shape
    size_y, size_z = share_y * py, share_z * pz
    fits = py == 4 and pz == 8 and fields == 4 and size_x % (128 * py) == 0
    if not fits or share_y % 16 or share_z % 8 or size_y != 8 * pz:
        return whole_shards(species, coupling, symbol_x, symbol_y, symbol_z)
    values = species.transpose(0, 2, 3, 1).reshape(fields, share_y * share_z, size_x)
    table_x = halves(mode_table(size_x))
    table_y = stack_left(mode_table(size_y))
    table_z = stack_left(mode_table(size_z))

    def swap(value, axis, count, k):
        return lax.ppermute(value, axis, [(i, i ^ k) for i in range(count)])

    spread = []
    for n, (first, count, _) in enumerate(CHUNKS):
        parts = along_x(values, table_x, first, count, py, n == 0)
        if n == 0:
            *parts, table_x = parts
        got = [parts[0]]
        for k in range(1, py):
            got.append(swap(parts[k], "py", py, k))
        spread.append(got)

    half = pz // 2
    blocks = []
    for n, (first, count, way) in enumerate(CHUNKS):
        if way == "direct":
            outs = [[k] for k in range(pz)]
        elif way == "relay":
            outs = [[2 * j, 2 * j + 1] for j in range(half)]
        else:
            outs = [[2 * j] for j in range(half)] + [[2 * j + 1 for j in range(half)]]
        parts = list(along_y(spread[n], table_y, share_z, pz, outs))
        if way == "direct":
            for k in range(1, pz):
                parts[k] = swap(parts[k], "pz", pz, k)
            blocks += [(parts[k], 0, k, first) for k in range(pz)]
            continue
        if way == "gather":
            other = swap(parts[half], "pz", pz, 1)
            merged = pack([[(parts[j], 0), (other, j)] for j in range(1, half)])
            blocks += [(parts[0], 0, 0, first), (other, 0, 1, first)]
            parts = [None] + list(merged)
        for j in range(1, half):
            parts[j] = swap(parts[j], "pz", pz, 2 * j)
        if way == "gather":
            blocks += [(parts[j], i, 2 * j + i, first) for j in range(1, half) for i in range(2)]
        else:
            blocks += [(parts[j], 0, 2 * j, first) for j in range(half)]
            other, = pack([[(parts[j], 1) for j in range(half)]])
            other = swap(other, "pz", pz, 1)
            blocks += [(other, j, 2 * j + 1, first) for j in range(half)]
    tie = [b[0] for b in blocks if b[2] == 0][-1]
    symbol_x, symbol_y, symbol_z, coupling, _ = lax.optimization_barrier(
        (symbol_x, symbol_y, symbol_z, coupling, tie))
    weight = own_weight(symbol_x, symbol_y, symbol_z, size_x // py, size_y // pz)
    coupling = jnp.broadcast_to(coupling[:, :, None, None], (fields, fields, 8, 128))
    start = CHUNKS[-1][0]
    early = along_z([block for block in blocks if block[3] < start], table_z, weight, coupling, fields)
    out = along_z_and_mix([block for block in blocks if block[3] >= start], table_z, early, weight, coupling)
    return out.transpose(0, 3, 1, 2)


def solution(mesh):
    py, pz = mesh.shape["py"], mesh.shape["pz"]

    def body(*args):
        return shards(*args, py=py, pz=pz)

    return jax.shard_map(
        body,
        mesh=mesh,
        in_specs=(P(None, None, "py", "pz"), P(), P(), P(), P()),
        out_specs=P(None, "py", "pz", None),
        check_vma=False,
    )
```

```python
import jax
import jax.numpy as jnp
import numpy as np
from jax import lax
from jax.experimental import pallas as pl
from jax.experimental.pallas import tpu as pltpu
from jax.sharding import PartitionSpec as P


CHUNKS = ((0, 12, 'relay'), (12, 20, 'direct'))
PIECES = 2
BF16, F32 = jnp.bfloat16, jnp.float32
VMEM = pl.BlockSpec(memory_space=pltpu.VMEM)


def mode_table(count):
    rank = np.arange(count)
    angle = np.pi / (4 * count) * ((2 * rank[:, None] + 1) * (2 * rank[None, :] + 1) % (8 * count))
    return np.cos(angle) * (2.0 / count) ** 0.5


def halves(table):
    high = table.astype(BF16)
    return np.stack([high, (table - high.astype(np.float64)).astype(BF16)])


def split(values):
    high = values.astype(BF16)
    return high, (values - high.astype(F32)).astype(BF16)


def dot(a, b):
    return jnp.dot(a, b, preferred_element_type=F32)


def stack_left(table):
    high, low = halves(table)
    return np.concatenate([high, high, low], axis=1)


def call(body, outs, scratch=(), flops=0, limit=24 << 20, **more):
    return pl.pallas_call(
        body,
        out_shape=outs,
        scratch_shapes=list(scratch),
        cost_estimate=pl.CostEstimate(flops=flops, bytes_accessed=1 << 20, transcendentals=0),
        compiler_params=pltpu.CompilerParams(vmem_limit_bytes=limit),
        **more,
    )


def along_x(values, table, lines, share_z, parts, load):
    rows, width = values.shape[1:]
    share_y = rows // share_z
    first = lines[0] // share_z
    fields = lines[-1] // share_z + 1 - first
    part = width // parts
    pieces = PIECES if load else 1
    depth = width // pieces

    def body(v_ref, h_ref, *refs):
        outs, r_ref = refs[:parts], refs[-1]
        copies = []
        if load:
            v_own, h_own, sems = refs[parts:parts + 3]
            for n in range(pieces):
                at = pl.ds(n * depth, depth)
                copies.append([
                    pltpu.make_async_copy(v_ref.at[:fields, :, at], v_own.at[:fields, :, at], sems.at[0, n]),
                    pltpu.make_async_copy(h_ref.at[:, at], h_own.at[:, at], sems.at[1, n]),
                ])
            copies.append([pltpu.make_async_copy(v_ref.at[fields:], v_own.at[fields:], sems.at[0, pieces])])
            for piece in copies:
                for copy in piece:
                    copy.start()
            v_ref, h_ref = v_own, h_own
        modes = 0.0
        for n in range(pieces):
            for copy in copies[n:n + 1] if load else []:
                copy[0].wait()
                copy[1].wait()
            at = slice(n * depth, (n + 1) * depth)
            high, low = split(v_ref[first:first + fields, :, at].reshape(fields * rows, depth))
            modes += dot(high, h_ref[0, at]) + dot(low, h_ref[0, at]) + dot(high, h_ref[1, at])
        for j in range(parts):
            r_ref[j] = modes[:, j * part:(j + 1) * part].reshape(fields, rows, part)
        me = lax.axis_index("py")
        for k in range(parts):
            for n, line in enumerate(lines):
                field, z = divmod(line, share_z)
                outs[k][n] = r_ref[me ^ k, field - first, pl.ds(z, share_y, stride=share_z), :]
        if load:
            copies[-1][0].wait()

    outs = [jax.ShapeDtypeStruct((len(lines), share_y, part), F32)] * parts
    scratch = [pltpu.VMEM((parts, fields, rows, part), F32)]
    space = VMEM
    if load:
        outs += [jax.ShapeDtypeStruct(values.shape, F32), jax.ShapeDtypeStruct(table.shape, BF16)]
        scratch = [pltpu.SemaphoreType.DMA((2, pieces + 1))] + scratch
        values = pltpu.with_memory_space_constraint(values, pltpu.HBM)
        table = pltpu.with_memory_space_constraint(table, pltpu.HBM)
        space = pl.BlockSpec(memory_space=pltpu.HBM)
    return call(
        body, outs, scratch, 6 * fields * rows * width * width, in_specs=[space, space], out_specs=[VMEM] * len(outs)
    )(values, table)


def along_y(arrived, table, parts, outs):
    sources = len(arrived)
    lines, share_y, lanes = arrived[0].shape
    size_y = sources * share_y
    out_y = size_y // parts

    def body(*refs):
        ins, h_ref = refs[:sources], refs[sources]
        out_refs = refs[sources + 1:-2]
        b_ref, r_ref = refs[-2:]
        me_y, me_z = lax.axis_index("py"), lax.axis_index("pz")
        for k in range(sources):
            start = (me_y ^ k) * share_y
            where = [pl.ds(pl.multiple_of(n * size_y + start, 16), share_y) for n in range(3)]
            for n in range(lines):
                high, low = split(ins[k][n])
                at = slice(n * lanes, (n + 1) * lanes)
                b_ref[where[0], at] = high
                b_ref[where[1], at] = low
                b_ref[where[2], at] = high
        r_ref[...] = dot(h_ref[...], b_ref[...])
        for blocks, ref in zip(outs, out_refs):
            for i, k in enumerate(blocks):
                where = pl.ds(pl.multiple_of((me_z ^ k) * out_y, 8), out_y)
                for n in range(lines):
                    ref[i, n] = r_ref[where, n * lanes:(n + 1) * lanes]

    wide = lines * lanes
    return call(
        body,
        [jax.ShapeDtypeStruct((len(blocks), lines, out_y, lanes), F32) for blocks in outs],
        [pltpu.VMEM((3 * size_y, wide), BF16), pltpu.VMEM((size_y, wide), F32)],
        6 * size_y * size_y * wide,
        in_specs=[VMEM] * (sources + 1),
        out_specs=[VMEM] * len(outs),
    )(*arrived, table)


def pack(outs):
    arrays = []
    for parts in outs:
        arrays += [a for a, _ in parts if not any(a is b for b in arrays)]
    place = [[([a is b for b in arrays].index(True), i) for a, i in parts] for parts in outs]

    def body(*refs):
        for parts, ref in zip(place, refs[len(arrays):]):
            for n, (a, i) in enumerate(parts):
                ref[n] = refs[a][i]

    return call(
        body,
        [jax.ShapeDtypeStruct((len(parts), *parts[0][0].shape[1:]), F32) for parts in outs],
        in_specs=[VMEM] * len(arrays),
        out_specs=[VMEM] * len(outs),
    )(*arrays)


def distinct(blocks):
    arrays = []
    for array, *_ in blocks:
        if not any(array is b for b in arrays):
            arrays.append(array)
    return arrays, [([array is b for b in arrays].index(True), *rest) for array, *rest in blocks]


def gather_z(place, ins, s_ref, first, share_y, share_z, pitch):
    me = lax.axis_index("pz")
    held = {line + n for a, _, _, line in place for n in range(ins[a].shape[1])}
    for field in range(s_ref.shape[0]):
        if not held.issuperset(range((first + field) * share_z, (first + field + 1) * share_z)):
            s_ref[field] = jnp.zeros(s_ref.shape[1:], F32)
    for a, index, k, line in place:
        start = (me ^ k) * share_z
        for n in range(ins[a].shape[1]):
            field, z = divmod(line + n, share_z)
            s_ref[field - first, pl.ds(start + z, share_y, stride=pitch), :] = ins[a][index, n]


def modes_z(h_ref, values):
    high, low = split(jnp.concatenate(values, axis=1))
    return dot(h_ref[...], jnp.concatenate([high, low, high], axis=0))


def scaled(c_ref, a, b, values):
    tile = c_ref[a, b]
    return (values.reshape(-1, *tile.shape) * tile[None]).reshape(values.shape)


def along_z(blocks, share_z, table, weight, coupling, early=None):
    arrays, place = distinct(blocks)
    lanes = arrays[0].shape[3]
    share_y, width = weight.shape[:2]
    fields = coupling.shape[0]
    first = min(line for *_, line in blocks) // share_z
    count = max((line + array.shape[1] - 1) // share_z for array, _, _, line in blocks) + 1 - first
    pitch = width + 8
    last = early is not None

    def body(*refs):
        ins = refs[:len(arrays)]
        h_ref, w_ref, c_ref = refs[len(arrays):len(arrays) + 3]
        if last:
            e_ref, out_ref, s_ref, o_ref, sems = refs[len(arrays) + 3:]
        else:
            o_ref, s_ref = refs[len(arrays) + 3:]
        gather_z(place, ins, s_ref, first, share_y, share_z, pitch)
        copies = []
        for y in range(share_y):
            modes = modes_z(h_ref, [s_ref[n, y * pitch:y * pitch + width] for n in range(count)])
            old = [modes[:, n * lanes:(n + 1) * lanes] for n in range(count)]
            w = w_ref[y]
            for a in range(fields):
                mixed = scaled(c_ref, a, first, old[0])
                for n in range(1, count):
                    mixed = mixed + scaled(c_ref, a, first + n, old[n])
                if first <= a < first + count:
                    mixed = mixed + w * (old[a - first] - mixed)
                else:
                    mixed = mixed - w * mixed
                o_ref[a, y] = e_ref[a, y] + mixed if last else mixed
            if last:
                copies.append(pltpu.make_async_copy(o_ref.at[:, y], out_ref.at[:, y], sems.at[y]))
                copies[-1].start()
        for copy in copies:
            copy.wait()

    shape = (fields, share_y, width, lanes)
    scratch = [pltpu.VMEM((count, share_y * pitch, lanes), F32)]
    if last:
        scratch += [pltpu.VMEM(shape, F32), pltpu.SemaphoreType.DMA((share_y,))]
    return call(
        body,
        jax.ShapeDtypeStruct(shape, F32),
        scratch,
        6 * share_y * width * width * lanes * count,
        in_specs=[VMEM] * (len(arrays) + 3 + last),
        out_specs=pl.BlockSpec(memory_space=pltpu.HBM) if last else VMEM,
    )(*arrays, table, weight, coupling, *([early] if last else []))


def transform_dim(values, dim):
    table = jnp.asarray(mode_table(values.shape[dim]), F32)
    moved = jnp.tensordot(values, table, axes=([dim], [0]), precision=lax.Precision.HIGHEST)
    return jnp.moveaxis(moved, -1, dim)


def own_weight(symbol_x, symbol_y, symbol_z, share_x, share_y):
    part_x = lax.dynamic_slice_in_dim(symbol_x, lax.axis_index("py") * share_x, share_x)
    part_y = lax.dynamic_slice_in_dim(symbol_y, lax.axis_index("pz") * share_y, share_y)
    symbol = part_x[None, None, :] + part_y[:, None, None] + symbol_z[None, :, None]
    return 1.0 / (1.0 + symbol)


def whole_shards(species, coupling, symbol_x, symbol_y, symbol_z):
    values = transform_dim(species, 1)
    values = lax.all_to_all(values, "py", split_axis=1, concat_axis=2, tiled=True)
    values = transform_dim(values, 2)
    values = lax.all_to_all(values, "pz", split_axis=2, concat_axis=3, tiled=True)
    values = transform_dim(values, 3)
    weight = own_weight(symbol_x, symbol_y, symbol_z, values.shape[1], values.shape[2])
    weight = weight.transpose(2, 0, 1)
    mixed = jnp.einsum("ab,bxyz->axyz", coupling, values, precision=lax.Precision.HIGHEST)
    return weight * values + (1.0 - weight) * mixed


def shards(species, coupling, symbol_x, symbol_y, symbol_z, py, pz):
    fields, size_x, share_y, share_z = species.shape
    size_y, size_z = share_y * py, share_z * pz
    fits = py == 4 and pz == 8 and fields == 4 and size_x % (128 * py) == 0
    if not fits or share_y % 16 or share_z % 8 or size_y != 8 * pz:
        return whole_shards(species, coupling, symbol_x, symbol_y, symbol_z)
    values = species.transpose(0, 2, 3, 1).reshape(fields, share_y * share_z, size_x)
    table_x = halves(mode_table(size_x))
    table_y = stack_left(mode_table(size_y))
    table_z = stack_left(mode_table(size_z))

    def swap(value, axis, count, k):
        return lax.ppermute(value, axis, [(i, i ^ k) for i in range(count)])

    spread = []
    for n, (first, count, _) in enumerate(CHUNKS):
        parts = along_x(values, table_x, range(first, first + count), share_z, py, n == 0)
        if n == 0:
            *parts, values, table_x = parts
        got = [parts[0]]
        for k in range(1, py):
            got.append(swap(parts[k], "py", py, k))
        spread.append(got)

    half = pz // 2
    blocks = []
    for n, (first, count, way) in enumerate(CHUNKS):
        if way == "direct":
            outs = [[k] for k in range(pz)]
        elif way == "relay":
            outs = [[2 * j, 2 * j + 1] for j in range(half)]
        else:
            outs = [[2 * j] for j in range(half)] + [[2 * j + 1 for j in range(half)]]
        parts = list(along_y(spread[n], table_y, pz, outs))
        if way == "direct":
            for k in range(1, pz):
                parts[k] = swap(parts[k], "pz", pz, k)
            blocks += [(parts[k], 0, k, first) for k in range(pz)]
            continue
        if way == "gather":
            other = swap(parts[half], "pz", pz, 1)
            merged = pack([[(parts[j], 0), (other, j)] for j in range(1, half)])
            blocks += [(parts[0], 0, 0, first), (other, 0, 1, first)]
            parts = [None] + list(merged)
        for j in range(1, half):
            parts[j] = swap(parts[j], "pz", pz, 2 * j)
        if way == "gather":
            blocks += [(parts[j], i, 2 * j + i, first) for j in range(1, half) for i in range(2)]
        else:
            blocks += [(parts[j], 0, 2 * j, first) for j in range(half)]
            other, = pack([[(parts[j], 1) for j in range(half)]])
            late = other
            other = swap(other, "pz", pz, 1)
            blocks += [(other, j, 2 * j + 1, first) for j in range(half)]
    symbol_x, symbol_y, symbol_z, coupling, _ = lax.optimization_barrier(
        (symbol_x, symbol_y, symbol_z, coupling, late))
    weight = own_weight(symbol_x, symbol_y, symbol_z, size_x // py, size_y // pz)
    coupling = jnp.broadcast_to(coupling[:, :, None, None], (fields, fields, 8, 128))
    start = CHUNKS[-1][0]
    early = along_z([block for block in blocks if block[3] < start], share_z, table_z, weight, coupling)
    out = along_z([block for block in blocks if block[3] >= start], share_z, table_z, weight, coupling, early)
    return out.transpose(0, 3, 1, 2)


def solution(mesh):
    py, pz = mesh.shape["py"], mesh.shape["pz"]

    def body(*args):
        return shards(*args, py=py, pz=pz)

    return jax.shard_map(
        body,
        mesh=mesh,
        in_specs=(P(None, None, "py", "pz"), P(), P(), P(), P()),
        out_specs=P(None, "py", "pz", None),
        check_vma=False,
    )
```

```python
import jax
import jax.numpy as jnp
import numpy as np
from jax import lax
from jax.experimental import pallas as pl
from jax.experimental.pallas import tpu as pltpu
from jax.sharding import PartitionSpec as P


CHUNKS = ((0, 12, 'relay'), (12, 20, 'direct'))
PIECES = 2
BF16, F32 = jnp.bfloat16, jnp.float32
VMEM = pl.BlockSpec(memory_space=pltpu.VMEM)


def mode_table(count):
    rank = np.arange(count)
    angle = np.pi / (4 * count) * ((2 * rank[:, None] + 1) * (2 * rank[None, :] + 1) % (8 * count))
    return np.cos(angle) * (2.0 / count) ** 0.5


def halves(table):
    high = table.astype(BF16)
    return np.stack([high, (table - high.astype(np.float64)).astype(BF16)])


def split(values):
    high = values.astype(BF16)
    return high, (values - high.astype(F32)).astype(BF16)


def dot(a, b):
    return jnp.dot(a, b, preferred_element_type=F32)


def stack_left(table):
    high, low = halves(table)
    return np.concatenate([high, high, low], axis=1)


def call(body, outs, scratch=(), flops=0, limit=24 << 20, **more):
    return pl.pallas_call(
        body,
        out_shape=outs,
        scratch_shapes=list(scratch),
        cost_estimate=pl.CostEstimate(flops=flops, bytes_accessed=1 << 20, transcendentals=0),
        compiler_params=pltpu.CompilerParams(vmem_limit_bytes=limit),
        **more,
    )


def along_x(values, table, lines, share_z, parts, load):
    rows, width = values.shape[1:]
    share_y = rows // share_z
    first = lines[0] // share_z
    fields = lines[-1] // share_z + 1 - first
    part = width // parts
    pieces = PIECES if load else 1
    depth = width // pieces

    def body(v_ref, h_ref, *refs):
        outs, r_ref = refs[:parts], refs[-1]
        copies = []
        if load:
            v_own, h_own, sems = refs[parts:parts + 3]
            for n in range(pieces):
                at = pl.ds(n * depth, depth)
                copies.append([
                    pltpu.make_async_copy(v_ref.at[:fields, :, at], v_own.at[:fields, :, at], sems.at[0, n]),
                    pltpu.make_async_copy(h_ref.at[:, at], h_own.at[:, at], sems.at[1, n]),
                ])
            copies.append([pltpu.make_async_copy(v_ref.at[fields:], v_own.at[fields:], sems.at[0, pieces])])
            for piece in copies:
                for copy in piece:
                    copy.start()
            v_ref, h_ref = v_own, h_own
        modes = 0.0
        for n in range(pieces):
            for copy in copies[n:n + 1] if load else []:
                copy[0].wait()
                copy[1].wait()
            at = slice(n * depth, (n + 1) * depth)
            high, low = split(v_ref[first:first + fields, :, at].reshape(fields * rows, depth))
            modes += dot(high, h_ref[0, at]) + dot(low, h_ref[0, at]) + dot(high, h_ref[1, at])
        for j in range(parts):
            r_ref[j] = modes[:, j * part:(j + 1) * part].reshape(fields, rows, part)
        me = lax.axis_index("py")
        for k in range(parts):
            for n, line in enumerate(lines):
                field, z = divmod(line, share_z)
                outs[k][n] = r_ref[me ^ k, field - first, pl.ds(z, share_y, stride=share_z), :]
        if load:
            copies[-1][0].wait()

    outs = [jax.ShapeDtypeStruct((len(lines), share_y, part), F32)] * parts
    scratch = [pltpu.VMEM((parts, fields, rows, part), F32)]
    space = VMEM
    if load:
        outs += [jax.ShapeDtypeStruct(values.shape, F32), jax.ShapeDtypeStruct(table.shape, BF16)]
        scratch = [pltpu.SemaphoreType.DMA((2, pieces + 1))] + scratch
        values = pltpu.with_memory_space_constraint(values, pltpu.HBM)
        table = pltpu.with_memory_space_constraint(table, pltpu.HBM)
        space = pl.BlockSpec(memory_space=pltpu.HBM)
    return call(
        body, outs, scratch, 6 * fields * rows * width * width, in_specs=[space, space], out_specs=[VMEM] * len(outs)
    )(values, table)


def along_y(arrived, table, parts, outs):
    sources = len(arrived)
    lines, share_y, lanes = arrived[0].shape
    size_y = sources * share_y
    out_y = size_y // parts

    def body(*refs):
        ins, h_ref = refs[:sources], refs[sources]
        out_refs = refs[sources + 1:-2]
        b_ref, r_ref = refs[-2:]
        me_y, me_z = lax.axis_index("py"), lax.axis_index("pz")
        for k in range(sources):
            start = (me_y ^ k) * share_y
            where = [pl.ds(pl.multiple_of(n * size_y + start, 16), share_y) for n in range(3)]
            for n in range(lines):
                high, low = split(ins[k][n])
                at = slice(n * lanes, (n + 1) * lanes)
                b_ref[where[0], at] = high
                b_ref[where[1], at] = low
                b_ref[where[2], at] = high
        r_ref[...] = dot(h_ref[...], b_ref[...])
        for blocks, ref in zip(outs, out_refs):
            for i, k in enumerate(blocks):
                where = pl.ds(pl.multiple_of((me_z ^ k) * out_y, 8), out_y)
                for n in range(lines):
                    ref[i, n] = r_ref[where, n * lanes:(n + 1) * lanes]

    wide = lines * lanes
    return call(
        body,
        [jax.ShapeDtypeStruct((len(blocks), lines, out_y, lanes), F32) for blocks in outs],
        [pltpu.VMEM((3 * size_y, wide), BF16), pltpu.VMEM((size_y, wide), F32)],
        6 * size_y * size_y * wide,
        in_specs=[VMEM] * (sources + 1),
        out_specs=[VMEM] * len(outs),
    )(*arrived, table)


def pack(outs):
    arrays = []
    for parts in outs:
        arrays += [a for a, _ in parts if not any(a is b for b in arrays)]
    place = [[([a is b for b in arrays].index(True), i) for a, i in parts] for parts in outs]

    def body(*refs):
        for parts, ref in zip(place, refs[len(arrays):]):
            for n, (a, i) in enumerate(parts):
                ref[n] = refs[a][i]

    return call(
        body,
        [jax.ShapeDtypeStruct((len(parts), *parts[0][0].shape[1:]), F32) for parts in outs],
        in_specs=[VMEM] * len(arrays),
        out_specs=[VMEM] * len(outs),
    )(*arrays)


def distinct(blocks):
    arrays = []
    for array, *_ in blocks:
        if not any(array is b for b in arrays):
            arrays.append(array)
    return arrays, [([array is b for b in arrays].index(True), *rest) for array, *rest in blocks]


def gather_z(place, ins, s_ref, first, share_y, share_z, pitch, around):
    me = lax.axis_index("pz")
    held = {(k % around, line + n) for a, _, k, line in place for n in range(ins[a].shape[1])}
    for field in range(s_ref.shape[0]):
        lines = range((first + field) * share_z, (first + field + 1) * share_z)
        if not held.issuperset((k, line) for k in range(around) for line in lines):
            s_ref[field] = jnp.zeros(s_ref.shape[1:], F32)
    for a, index, k, line in place:
        start = (me ^ k) % around * share_z
        for n in range(ins[a].shape[1]):
            field, z = divmod(line + n, share_z)
            s_ref[field - first, pl.ds(start + z, share_y, stride=pitch), :] = ins[a][index, n]


def modes_z(h, values):
    high, low = split(jnp.concatenate(values, axis=1))
    return dot(h, jnp.concatenate([high, low, high], axis=0))


def scaled(c_ref, a, b, values):
    tile = c_ref[a, b]
    return (values.reshape(-1, *tile.shape) * tile[None]).reshape(values.shape)


def along_z(blocks, share_z, table, weight, coupling, early=None):
    arrays, place = distinct(blocks)
    lanes = arrays[0].shape[3]
    share_y, width = weight.shape[:2]
    fields = coupling.shape[0]
    first = min(line for *_, line in blocks) // share_z
    count = max((line + array.shape[1] - 1) // share_z for array, _, _, line in blocks) + 1 - first
    last = early is not None
    parts = width // share_z
    around = parts // 2 if last else parts
    depth = around * share_z
    pitch = depth + 8

    def body(*refs):
        ins = refs[:len(arrays)]
        h_ref, w_ref, c_ref = refs[len(arrays):len(arrays) + 3]
        if last:
            e_ref, out_ref, s_ref, o_ref, sems = refs[len(arrays) + 3:]
        else:
            o_ref, s_ref = refs[len(arrays) + 3:]
        gather_z(place, ins, s_ref, first, share_y, share_z, pitch, around)
        h = h_ref[1 - lax.axis_index("pz") // around if last else 0]
        copies = []
        for y in range(share_y):
            modes = modes_z(h, [s_ref[n, y * pitch:y * pitch + depth] for n in range(count)])
            old = [modes[:, n * lanes:(n + 1) * lanes] for n in range(count)]
            w = w_ref[y]
            for a in range(fields):
                mixed = scaled(c_ref, a, first, old[0])
                for n in range(1, count):
                    mixed = mixed + scaled(c_ref, a, first + n, old[n])
                if first <= a < first + count:
                    mixed = mixed + w * (old[a - first] - mixed)
                else:
                    mixed = mixed - w * mixed
                o_ref[a, y] = e_ref[a, y] + mixed if last else mixed
            if last:
                copies.append(pltpu.make_async_copy(o_ref.at[:, y], out_ref.at[:, y], sems.at[y]))
                copies[-1].start()
        for copy in copies:
            copy.wait()

    shape = (fields, share_y, width, lanes)
    scratch = [pltpu.VMEM((count, share_y * pitch, lanes), F32)]
    if last:
        scratch += [pltpu.VMEM(shape, F32), pltpu.SemaphoreType.DMA((share_y,))]
    return call(
        body,
        jax.ShapeDtypeStruct(shape, F32),
        scratch,
        6 * share_y * width * width * lanes * count,
        in_specs=[VMEM] * (len(arrays) + 3 + last),
        out_specs=pl.BlockSpec(memory_space=pltpu.HBM) if last else VMEM,
    )(*arrays, table, weight, coupling, *([early] if last else []))


def transform_dim(values, dim):
    table = jnp.asarray(mode_table(values.shape[dim]), F32)
    moved = jnp.tensordot(values, table, axes=([dim], [0]), precision=lax.Precision.HIGHEST)
    return jnp.moveaxis(moved, -1, dim)


def own_weight(symbol_x, symbol_y, symbol_z, share_x, share_y):
    part_x = lax.dynamic_slice_in_dim(symbol_x, lax.axis_index("py") * share_x, share_x)
    part_y = lax.dynamic_slice_in_dim(symbol_y, lax.axis_index("pz") * share_y, share_y)
    symbol = part_x[None, None, :] + part_y[:, None, None] + symbol_z[None, :, None]
    return 1.0 / (1.0 + symbol)


def whole_shards(species, coupling, symbol_x, symbol_y, symbol_z):
    values = transform_dim(species, 1)
    values = lax.all_to_all(values, "py", split_axis=1, concat_axis=2, tiled=True)
    values = transform_dim(values, 2)
    values = lax.all_to_all(values, "pz", split_axis=2, concat_axis=3, tiled=True)
    values = transform_dim(values, 3)
    weight = own_weight(symbol_x, symbol_y, symbol_z, values.shape[1], values.shape[2])
    weight = weight.transpose(2, 0, 1)
    mixed = jnp.einsum("ab,bxyz->axyz", coupling, values, precision=lax.Precision.HIGHEST)
    return weight * values + (1.0 - weight) * mixed


def shards(species, coupling, symbol_x, symbol_y, symbol_z, py, pz):
    fields, size_x, share_y, share_z = species.shape
    size_y, size_z = share_y * py, share_z * pz
    fits = py == 4 and pz == 8 and fields == 4 and size_x % (128 * py) == 0
    if not fits or share_y % 16 or share_z % 8 or size_y != 8 * pz:
        return whole_shards(species, coupling, symbol_x, symbol_y, symbol_z)
    values = species.transpose(0, 2, 3, 1).reshape(fields, share_y * share_z, size_x)
    table_x = halves(mode_table(size_x))
    table_y = stack_left(mode_table(size_y))
    table_z = stack_left(mode_table(size_z))[None]
    halves_z = np.stack([stack_left(h) for h in np.split(mode_table(size_z), 2, axis=1)])

    def swap(value, axis, count, k):
        return lax.ppermute(value, axis, [(i, i ^ k) for i in range(count)])

    spread = []
    for n, (first, count, _) in enumerate(CHUNKS):
        parts = along_x(values, table_x, range(first, first + count), share_z, py, n == 0)
        if n == 0:
            *parts, values, table_x = parts
        got = [parts[0]]
        for k in range(1, py):
            got.append(swap(parts[k], "py", py, k))
        spread.append(got)

    half = pz // 2
    blocks = []
    for n, (first, count, way) in enumerate(CHUNKS):
        if way == "direct":
            outs = [[k] for k in range(pz)]
        elif way == "relay":
            outs = [[2 * j, 2 * j + 1] for j in range(half)]
        else:
            outs = [[2 * j] for j in range(half)] + [[2 * j + 1 for j in range(half)]]
        parts = list(along_y(spread[n], table_y, pz, outs))
        if way == "direct":
            for k in range(1, pz):
                parts[k] = swap(parts[k], "pz", pz, k)
            blocks += [(parts[k], 0, k, first) for k in range(pz)]
            continue
        if way == "gather":
            other = swap(parts[half], "pz", pz, 1)
            merged = pack([[(parts[j], 0), (other, j)] for j in range(1, half)])
            blocks += [(parts[0], 0, 0, first), (other, 0, 1, first)]
            parts = [None] + list(merged)
        for j in range(1, half):
            parts[j] = swap(parts[j], "pz", pz, 2 * j)
        if way == "gather":
            blocks += [(parts[j], i, 2 * j + i, first) for j in range(1, half) for i in range(2)]
        else:
            blocks += [(parts[j], 0, 2 * j, first) for j in range(half)]
            other, = pack([[(parts[j], 1) for j in range(half)]])
            late = other
            other = swap(other, "pz", pz, 1)
            blocks += [(other, j, 2 * j + 1, first) for j in range(half)]
    symbol_x, symbol_y, symbol_z, coupling, _ = lax.optimization_barrier(
        (symbol_x, symbol_y, symbol_z, coupling, late))
    weight = own_weight(symbol_x, symbol_y, symbol_z, size_x // py, size_y // pz)
    coupling = jnp.broadcast_to(coupling[:, :, None, None], (fields, fields, 8, 128))
    start = CHUNKS[-1][0]
    final = [block for block in blocks if block[3] >= start and block[2] >= half]
    rest = [block for block in blocks if block[3] < start or block[2] < half]
    early = along_z(rest, share_z, table_z, weight, coupling)
    out = along_z(final, share_z, halves_z, weight, coupling, early)
    return out.transpose(0, 3, 1, 2)


def solution(mesh):
    py, pz = mesh.shape["py"], mesh.shape["pz"]

    def body(*args):
        return shards(*args, py=py, pz=pz)

    return jax.shard_map(
        body,
        mesh=mesh,
        in_specs=(P(None, None, "py", "pz"), P(), P(), P(), P()),
        out_specs=P(None, "py", "pz", None),
        check_vma=False,
    )
```
